128 devices in a mesh: row: 8 (over y, core), col: 16 (over z, x).
Axes of the slice: x: 4, y: 4, z: 4, core: 2. Of those that a mesh axis runs over, the one named last changes fastest.
Arguments:
- parent_front: float32 [8, 2048, 4, 4096], P(None, 'row', None, 'col'), may hold values from -6 to 6
- generators: bfloat16 [96, 256, 256], P('row'), may hold values from -1.5 to 1.5
- diagonal_blocks: bfloat16 [96, 256, 256], P('row'), may hold values from -6 to 6
- coupling: bfloat16 [2, 256, 256], replicated, may hold values from -0.375 to 0.375
- block_map: int32 [2, 48], replicated, may hold values from 0 to 63, as said below
- valid_rows: int32 [2, 48], replicated, may hold values from 128 to 256
Outputs:
- assembled: float32 [8, 2048, 4, 4096], P(None, 'row', None, 'col')
The draws below stay inside these ranges and needn't reach their ends.
Inputs may be any that keep to these rules, and one draw needn't show every extreme that they name: `block_map`: for each child c and each s < 4, the child blocks s * 12 to (s + 1) * 12 - 1 map in increasing order to distinct parent blocks of the range s * 16 to (s + 1) * 16 - 1, and the parent blocks s * 16 + m * 8 of that range always receive one.
All inputs are finite; a program needn't handle non-finite values.
Results may differ from the reference program's by a relative error of at most 0.0028.
Values may be sent and summed in bfloat16 or wider, within the bound.
No kernel may reach another device: no remote copies, remote signals or barrier semaphores. Data moves between devices by JAX's collectives and lax.ppermute only.
A program may use at most 128 MiB of HBM per device.

```python
import jax
import jax.numpy as jnp
from jax import lax

BLK = 256
RANK = 256
BR_DEV = 8
PB = 64
BC_DEV = 4
WIN = 16
CG = 12
HALF = 4
CB = 48
N_ROW = 8
N_COL = 16


def draw_block_map(key, part):
    child_rows = []
    for child_index in range(2):
        pieces = []
        for group_index in range(HALF):
            window_key = jax.random.fold_in(key, 1000 * child_index + group_index + 17)
            offsets = jnp.arange(WIN, dtype=jnp.int32)
            scores = jax.random.randint(window_key, (WIN,), 0, 1 << 20, dtype=jnp.int32) * WIN + offsets
            scores = jnp.where(offsets % N_ROW == 0, jnp.int32(1 << 30), scores)
            gap_order = jnp.argsort(scores, stable=True)
            gap_slots = gap_order[:WIN - CG]
            gap_flags = jnp.zeros((WIN,), jnp.int32).at[gap_slots].set(1)
            sorted_slots = jnp.argsort(gap_flags * WIN + offsets, stable=True).astype(jnp.int32)
            chosen = sorted_slots[:CG] + WIN * group_index
            pieces.append(chosen)
        child_rows.append(jnp.concatenate(pieces))
    return jnp.stack(child_rows).astype(jnp.int32)


def place_ends(entries, own_key, low, high):
    longest = entries.shape.index(max(entries.shape))
    spots = []
    for shift in (0, 1):
        where = [jax.random.randint(jax.random.fold_in(own_key, axis), (), 0, length) for axis, length in enumerate(entries.shape)]
        where[longest] = (where[longest] + shift) % entries.shape[longest]
        spots.append(tuple(where))
    return entries.at[spots[0]].set(low).at[spots[1]].set(high)


def shard_levels(own_key, extent, cuts, smallest, largest):
    def one(dim, blocks):
        heights = jax.random.uniform(jax.random.fold_in(jax.random.fold_in(own_key, 6), dim), (blocks,), jnp.float32, smallest / len(cuts), largest / len(cuts))
        return jnp.repeat(jnp.exp(heights), extent[dim] // blocks).reshape((-1,) + (1,) * (len(extent) - dim - 1))

    loudness = one(*cuts[0])
    for cut in cuts[1:]:
        loudness = loudness * one(*cut)
    return loudness


def bell_draw(stream_key, dims, scale, reach, cuts=(), held_as=jnp.bfloat16):
    entries = jax.random.normal(stream_key, dims, jnp.float32) * scale
    if len(cuts) > 0:
        entries = shard_levels(stream_key, dims, cuts, -0.22, 0.18) * entries
    return jnp.clip(entries, min=-reach, max=reach).astype(held_as)


def setup_inputs(seed: int = 0) -> dict:
    arg_keys = jax.random.split(jax.random.key(seed), 7)
    parent_front = bell_draw(arg_keys[0], (BR_DEV, N_ROW * BLK, BC_DEV, N_COL * BLK), 1.0, 6.0, ((1, 8), (3, 16)), jnp.float32)
    generators = bell_draw(arg_keys[1], (2 * CB, BLK, RANK), 0.25, 1.5, ((0, 8),))
    diagonal_blocks = bell_draw(arg_keys[2], (2 * CB, BLK, BLK), 1.0, 6.0, ((0, 8),))
    coupling = bell_draw(arg_keys[3], (2, RANK, RANK), RANK ** -0.5, 0.375)
    block_map = draw_block_map(jax.random.fold_in(arg_keys[6], 71), 0)
    valid_rows = place_ends(jax.random.randint(arg_keys[5], (2, CB), BLK // 2, BLK + 1), jax.random.fold_in(arg_keys[5], 1), BLK // 2, BLK).astype(jnp.int32)
    return dict(parent_front=parent_front, generators=generators, diagonal_blocks=diagonal_blocks, coupling=coupling, block_map=block_map, valid_rows=valid_rows)


def child_select(stacked, child_index):
    grouped = stacked.reshape((HALF, 2, CG) + stacked.shape[1:])
    return grouped[:, child_index].reshape((CB,) + stacked.shape[1:])


def child_parts(gen_blocks, diag_rows, coupling_one, map_row, count_row):
    row_offsets = jnp.arange(BLK, dtype=jnp.int32)
    kept_mask = (row_offsets[None, :] < count_row[:, None]).astype(jnp.float32)
    masked = gen_blocks.astype(jnp.float32) * kept_mask[:, :, None]
    projected = jnp.einsum("ixq,qr->ixr", masked, coupling_one.astype(jnp.float32)).astype(jnp.bfloat16)
    diag_kept = diag_rows.astype(jnp.float32) * kept_mask[:, :, None] * kept_mask[:, None, :]
    placing = (map_row[None, :] == jnp.arange(PB, dtype=jnp.int32)[:, None]).astype(jnp.float32)
    placed_gen = jnp.einsum("pi,ixq->pxq", placing, masked)
    placed_proj = jnp.einsum("pi,ixq->pxq", placing, projected.astype(jnp.float32))
    placed_diag = jnp.einsum("pi,ixz->pxz", placing, diag_kept)
    return placed_gen, placed_proj, placed_diag


def reference(parent_front, generators, diagonal_blocks, coupling, block_map, valid_rows):
    front_blocks = parent_front.reshape(PB, BLK, PB, BLK)
    child_data = [child_parts(child_select(generators, child_index),
                              child_select(diagonal_blocks, child_index),
                              coupling[child_index], block_map[child_index], valid_rows[child_index])
                  for child_index in range(2)]
    placed_gen = jnp.stack([child_data[0][0], child_data[1][0]], axis=1)
    placed_proj = jnp.stack([child_data[0][1], child_data[1][1]])
    placed_diag = jnp.stack([child_data[0][2], child_data[1][2]], axis=1)
    block_ids = jnp.arange(PB, dtype=jnp.int32)

    def one_row(row_items):
        front_row, gen_row, diag_row, row_id = row_items
        on_diag = (block_ids == row_id).astype(jnp.float32)
        running = front_row
        for child_index in range(2):
            child_tile = jnp.einsum("xq,jzq->xjz", gen_row[child_index], placed_proj[child_index])
            child_tile = child_tile + diag_row[child_index][:, None, :] * on_diag[None, :, None]
            rounded = lax.optimization_barrier(child_tile.astype(jnp.bfloat16))
            running = running + rounded.astype(jnp.float32)
        return running

    rows_out = lax.map(one_row, (front_blocks, placed_gen, placed_diag, block_ids))
    return rows_out.reshape(BR_DEV, N_ROW * BLK, BC_DEV, N_COL * BLK)
```

```python
import functools

import jax
import jax.numpy as jnp
from jax import lax
from jax.experimental import pallas as pl
from jax.experimental.pallas import tpu as pltpu
from jax.sharding import PartitionSpec as P

Y, Z, X, BLK = 4, 4, 4, 256
QUART = BLK // 8
WIN, CG = 16, 12


def pairs(move):
    out = []
    for y in range(Y):
        for k in range(2):
            for z in range(Z):
                for x in range(X):
                    b = move(y, k, z, x)
                    source = (2 * y + k) * Z * X + z * X + x
                    target = (2 * (b[0] % Y) + b[1]) * Z * X + (b[2] % Z) * X + b[3] % X
                    out.append((source, target))
    return out


def shift(value, move):
    return lax.ppermute(value, ("row", "col"), pairs(move))


def where_am_i():
    row = lax.axis_index("row")
    col = lax.axis_index("col")
    return row // 2, row % 2, col // X, col % X


def keep(count, start, rows):
    ids = lax.broadcasted_iota(jnp.int32, (rows, BLK), 0) + start
    return ids < count


def pack_kernel(map_ref, count_ref, gen_ref, diag_ref, coup_ref, loc_ref, rem_ref, send_ref, col_ref):
    y, k, z, x = where_am_i()
    zero = jnp.zeros((), jnp.bfloat16)
    loc_ref[...] = jnp.zeros_like(loc_ref)
    rem_ref[...] = jnp.zeros_like(rem_ref)
    send_ref[...] = jnp.zeros_like(send_ref)
    col_ref[...] = jnp.zeros_like(col_ref)
    t = z * X + x

    def one(i, carry):
        w = map_ref[k, y * CG + i] - y * WIN
        count = count_ref[k, y * CG + i]
        mine = lax.rem(w, 2) == k
        j = w // 2
        m = j // 4
        step = lax.rem(lax.rem(j, 4) - y + 4, 4)

        @pl.when(step == 0)
        def _():
            full = jnp.where(keep(count, 0, BLK), gen_ref[i], zero)

            @pl.when(mine)
            def _():
                loc_ref[m] = full

            @pl.when(jnp.logical_not(mine))
            def _():
                for part in range(4):
                    send_ref[6 + 4 * m + part] = full[64 * part : 64 * part + 64]

        @pl.when(step > 0)
        def _():
            parts = []
            for start in (QUART * x, BLK // 2 + QUART * z):
                start = pl.multiple_of(start, QUART)
                piece = gen_ref[i, pl.ds(start, QUART), :]
                parts.append(jnp.where(keep(count, start, QUART), piece, zero))

            @pl.when(mine)
            def _():
                rem_ref[step - 1, 0, m] = parts[0]
                rem_ref[step - 1, 1, m] = parts[1]

            @pl.when(jnp.logical_not(mine))
            def _():
                send_ref[2 * (step - 1) + m, :QUART] = parts[0]
                send_ref[2 * (step - 1) + m, QUART:] = parts[1]

        @pl.when(w == t)
        def _():
            full = jnp.where(keep(count, 0, BLK), gen_ref[i], zero)
            col_ref[0] = lax.dot_general(
                coup_ref[k], full, (((0,), (1,)), ((), ())), preferred_element_type=jnp.float32
            ).astype(jnp.bfloat16)
            lanes = lax.broadcasted_iota(jnp.int32, (BLK, BLK), 1) < count
            col_ref[1] = jnp.where(keep(count, 0, BLK) & lanes, diag_ref[i], zero)

        return carry

    lax.fori_loop(0, CG, one, 0)


def join_kernel(
    par_ref, loc_ref, swap_ref, r1, r2, r3, x1, x2, x3, z1, z2, z3,
    c0, c1, c2, c3, d0, d1, d2, d3, out_ref, rows_ref, cols_ref,
):
    y, k, z, x = where_am_i()
    a = pl.program_id(0)
    own = (c0, c1, c2, c3)
    other = (d0, d1, d2, d3)

    @pl.when(a == 0)
    def _():
        for m in range(2):
            rows_ref[2 * y + m, :, :BLK] = loc_ref[m]
            for part in range(4):
                rows_ref[2 * y + m, 64 * part : 64 * part + 64, BLK:] = swap_ref[6 + 4 * m + part]
        for step, got in ((1, r1), (2, r2), (3, r3)):
            s = lax.rem(y - step + 4, 4)
            for child in range(2):
                for m in range(2):
                    lanes = slice(BLK * child, BLK * child + BLK)
                    b = 2 * child + m
                    at = pl.multiple_of(QUART * x, QUART)
                    rows_ref[2 * s + m, pl.ds(at, QUART), lanes] = got[0, b]
                    at = pl.multiple_of(BLK // 2 + QUART * z, QUART)
                    rows_ref[2 * s + m, pl.ds(at, QUART), lanes] = got[1, b]
                    for far, gx, gz in ((1, x1, z1), (2, x2, z2), (3, x3, z3)):
                        at = pl.multiple_of(QUART * lax.rem(x - far + 4, 4), QUART)
                        rows_ref[2 * s + m, pl.ds(at, QUART), lanes] = gx[step - 1, b]
                        at = pl.multiple_of(BLK // 2 + QUART * lax.rem(z - far + 4, 4), QUART)
                        rows_ref[2 * s + m, pl.ds(at, QUART), lanes] = gz[step - 1, b]
        for step in range(4):
            s = lax.rem(y - step + 4, 4)
            cols_ref[s, :BLK] = own[step][0]
            cols_ref[s, BLK:] = other[step][0]

    left = rows_ref[a]
    for b in range(4):
        tile = jnp.dot(left, cols_ref[b], preferred_element_type=jnp.float32)
        for half in range(2):
            at = pl.ds(4 * half + b, BLK, stride=8)
            out_ref[0, at, :] = par_ref[0, at, :] + tile[:, 128 * half : 128 * half + 128]

    t = z * X + x
    row = 2 * y + k

    @pl.when((row == lax.rem(t, 8)) & (lax.rem(a, 2) == t // 8))
    def _():
        for step in range(4):

            @pl.when(lax.rem(y - step + 4, 4) == a // 2)
            def _():
                both = own[step][1].astype(jnp.float32) + other[step][1].astype(jnp.float32)
                for half in range(2):
                    at = pl.ds(4 * half + a // 2, BLK, stride=8)
                    out_ref[0, at, :] = out_ref[0, at, :] + both[:, 128 * half : 128 * half + 128]


def shards(parent_front, generators, diagonal_blocks, coupling, block_map, valid_rows):
    bf16 = jnp.bfloat16
    vmem = pl.BlockSpec(memory_space=pltpu.VMEM)
    smem = pl.BlockSpec(memory_space=pltpu.SMEM)
    loc, rem, send, col = pl.pallas_call(
        pack_kernel,
        out_shape=(
            jax.ShapeDtypeStruct((2, BLK, BLK), bf16),
            jax.ShapeDtypeStruct((3, 2, 2, QUART, BLK), bf16),
            jax.ShapeDtypeStruct((14, 2 * QUART, BLK), bf16),
            jax.ShapeDtypeStruct((2, BLK, BLK), bf16),
        ),
        in_specs=[smem, smem, vmem, vmem, vmem],
        out_specs=(vmem, vmem, vmem, vmem),
        compiler_params=pltpu.CompilerParams(vmem_limit_bytes=16 * 2**20),
    )(block_map, valid_rows, generators, diagonal_blocks, coupling)

    flip = lambda y, k, z, x: (y, 1 - k, z, x)
    swap = shift(send, flip)
    got = []
    for step in (1, 3, 2):
        there = swap[2 * step - 2 : 2 * step].reshape(2, 2, QUART, BLK).swapaxes(0, 1)
        payload = jnp.concatenate([rem[step - 1], there], axis=1)
        got.append(shift(payload, lambda y, k, z, x, n=step: (y + n, k, z, x)))
    got = [got[0], got[2], got[1]]
    cols = [col] + [shift(col, lambda y, k, z, x, n=step: (y + n, k, z, x)) for step in (1, 2, 3)]
    others = [shift(c, flip) for c in cols]
    for_x = jnp.stack([g[0] for g in got])
    for_z = jnp.stack([g[1] for g in got])
    xs = [shift(for_x, lambda y, k, z, x, n=far: (y, k, z, x + n)) for far in (1, 2, 3)]
    zs = [shift(for_z, lambda y, k, z, x, n=far: (y, k, z + n, x)) for far in (1, 2, 3)]

    a_count = parent_front.shape[0]
    flat = parent_front.reshape(a_count, BLK, 4, 2, 128).transpose(0, 1, 3, 2, 4).reshape(a_count, BLK * 8, 128)
    block = pl.BlockSpec((1, BLK * 8, 128), lambda a: (a, 0, 0))
    joined = pl.pallas_call(
        join_kernel,
        grid=(a_count,),
        out_shape=jax.ShapeDtypeStruct(flat.shape, jnp.float32),
        in_specs=[block] + [vmem] * 19,
        out_specs=block,
        scratch_shapes=[
            pltpu.VMEM((a_count, BLK, 2 * BLK), bf16),
            pltpu.VMEM((4, 2 * BLK, BLK), bf16),
        ],
        compiler_params=pltpu.CompilerParams(vmem_limit_bytes=32 * 2**20),
    )(flat, loc, swap, *got, *xs, *zs, *cols, *others)
    return joined.reshape(a_count, BLK, 2, 4, 128).transpose(0, 1, 3, 2, 4).reshape(parent_front.shape)


def solution(mesh):
    in_specs = (P(None, "row", None, "col"), P("row", None, None), P("row", None, None), P(), P(), P())
    out_specs = P(None, "row", None, "col")
    return jax.shard_map(shards, mesh=mesh, in_specs=in_specs, out_specs=out_specs, check_vma=False)
```

```python
import jax
import jax.numpy as jnp
from jax import lax
from jax.experimental import pallas as pl
from jax.experimental.pallas import tpu as pltpu
from jax.sharding import PartitionSpec as P


Y, Z, X, BLK = 4, 4, 4, 256
QUART = BLK // 8
WIN, CG = 16, 12


def pairs(move):
    out = []
    for y in range(Y):
        for k in range(2):
            for z in range(Z):
                for x in range(X):
                    b = move(y, k, z, x)
                    source = (2 * y + k) * Z * X + z * X + x
                    target = (2 * (b[0] % Y) + b[1]) * Z * X + (b[2] % Z) * X + b[3] % X
                    out.append((source, target))
    return out


def shift(value, move):
    return lax.ppermute(value, ("row", "col"), pairs(move))


def where_am_i():
    row = lax.axis_index("row")
    col = lax.axis_index("col")
    return row // 2, row % 2, col // X, col % X


def keep(count, start, rows):
    ids = lax.broadcasted_iota(jnp.int32, (rows, BLK), 0) + start
    return ids < count


def rows_kernel(map_hbm, count_hbm, gen_hbm, loc_ref, rem_ref, send_ref, map_ref, count_ref, gen_ref, sems):
    y, k, z, x = where_am_i()
    copies = [
        pltpu.make_async_copy(map_hbm, map_ref, sems.at[0]),
        pltpu.make_async_copy(count_hbm, count_ref, sems.at[1]),
        pltpu.make_async_copy(gen_hbm, gen_ref, sems.at[2]),
    ]
    for copy in copies:
        copy.start()
    zero = jnp.zeros((), jnp.bfloat16)
    loc_ref[...] = jnp.zeros_like(loc_ref)
    rem_ref[...] = jnp.zeros_like(rem_ref)
    send_ref[...] = jnp.zeros_like(send_ref)
    for copy in copies:
        copy.wait()

    def one(i, carry):
        w = map_ref[k, y * CG + i] - y * WIN
        count = count_ref[k, y * CG + i]
        mine = lax.rem(w, 2) == k
        j = w // 2
        m = j // 4
        step = lax.rem(lax.rem(j, 4) - y + 4, 4)

        @pl.when(step == 0)
        def _():
            full = jnp.where(keep(count, 0, BLK), gen_ref[i], zero)

            @pl.when(mine)
            def _():
                loc_ref[m] = full

            @pl.when(jnp.logical_not(mine))
            def _():
                for part in range(4):
                    send_ref[6 + 4 * m + part] = full[64 * part : 64 * part + 64]

        @pl.when(step > 0)
        def _():
            parts = []
            for start in (QUART * x, BLK // 2 + QUART * z):
                start = pl.multiple_of(start, QUART)
                piece = gen_ref[i, pl.ds(start, QUART), :]
                parts.append(jnp.where(keep(count, start, QUART), piece, zero))

            @pl.when(mine)
            def _():
                rem_ref[step - 1, 0, m] = parts[0]
                rem_ref[step - 1, 1, m] = parts[1]

            @pl.when(jnp.logical_not(mine))
            def _():
                send_ref[2 * (step - 1) + m, :QUART] = parts[0]
                send_ref[2 * (step - 1) + m, QUART:] = parts[1]

        return carry

    lax.fori_loop(0, CG, one, 0)


def column_kernel(map_hbm, count_hbm, gen_hbm, diag_hbm, coup_hbm, col_ref, map_ref, count_ref, gen_ref, diag_ref, coup_ref, sems):
    y, k, z, x = where_am_i()
    target = y * WIN + z * X + x
    coup = pltpu.make_async_copy(coup_hbm.at[k], coup_ref, sems.at[2])
    coup.start()
    tables = [
        pltpu.make_async_copy(map_hbm, map_ref, sems.at[0]),
        pltpu.make_async_copy(count_hbm, count_ref, sems.at[1]),
    ]
    for copy in tables:
        copy.start()
    for copy in tables:
        copy.wait()
    which = jnp.int32(0)
    count = jnp.int32(0)
    for i in range(CG):
        hit = map_ref[k, y * CG + i] == target
        which = jnp.where(hit, i, which)
        count = jnp.where(hit, count_ref[k, y * CG + i], count)
    blocks = [
        pltpu.make_async_copy(gen_hbm.at[which], gen_ref, sems.at[3]),
        pltpu.make_async_copy(diag_hbm.at[which], diag_ref, sems.at[4]),
    ]
    for copy in blocks:
        copy.start()
    coup.wait()
    for copy in blocks:
        copy.wait()
    zero = jnp.zeros((), jnp.bfloat16)
    full = jnp.where(keep(count, 0, BLK), gen_ref[...], zero)
    col_ref[0] = lax.dot_general(
        coup_ref[...], full, (((0,), (1,)), ((), ())), preferred_element_type=jnp.float32
    ).astype(jnp.bfloat16)
    lanes = lax.broadcasted_iota(jnp.int32, (BLK, BLK), 1) < count
    col_ref[1] = jnp.where(keep(count, 0, BLK) & lanes, diag_ref[...], zero)


def fetch_kernel(par_ref, out_ref):
    a = pl.program_id(0)
    for b in range(4):
        for half in range(2):
            out_ref[a, b, :, 128 * half : 128 * half + 128] = par_ref[0, pl.ds(4 * half + b, BLK, stride=8), :]


def join_kernel(
    par_ref, loc_ref, swap_ref, r1, r2, r3, x1, x2, x3, z1, z2, z3,
    c0, c1, c2, c3, d0, d1, d2, d3, out_ref, rows_ref, cols_ref,
):
    y, k, z, x = where_am_i()
    a = pl.program_id(0)
    own = (c0, c1, c2, c3)
    other = (d0, d1, d2, d3)

    @pl.when(a == 0)
    def _():
        for m in range(2):
            rows_ref[2 * y + m, :, :BLK] = loc_ref[m]
            for part in range(4):
                rows_ref[2 * y + m, 64 * part : 64 * part + 64, BLK:] = swap_ref[6 + 4 * m + part]
        for step, got in ((1, r1), (2, r2), (3, r3)):
            s = lax.rem(y - step + 4, 4)
            for child in range(2):
                for m in range(2):
                    lanes = slice(BLK * child, BLK * child + BLK)
                    b = 2 * child + m
                    at = pl.multiple_of(QUART * x, QUART)
                    rows_ref[2 * s + m, pl.ds(at, QUART), lanes] = got[0, b]
                    at = pl.multiple_of(BLK // 2 + QUART * z, QUART)
                    rows_ref[2 * s + m, pl.ds(at, QUART), lanes] = got[1, b]
                    for far, gx, gz in ((1, x1, z1), (2, x2, z2), (3, x3, z3)):
                        at = pl.multiple_of(QUART * lax.rem(x - far + 4, 4), QUART)
                        rows_ref[2 * s + m, pl.ds(at, QUART), lanes] = gx[step - 1, b]
                        at = pl.multiple_of(BLK // 2 + QUART * lax.rem(z - far + 4, 4), QUART)
                        rows_ref[2 * s + m, pl.ds(at, QUART), lanes] = gz[step - 1, b]
        for step in range(4):
            s = lax.rem(y - step + 4, 4)
            cols_ref[s, :BLK] = own[step][0]
            cols_ref[s, BLK:] = other[step][0]

    left = rows_ref[a]
    for b in range(4):
        tile = par_ref[a, b] + jnp.dot(left, cols_ref[b], preferred_element_type=jnp.float32)
        for half in range(2):
            at = pl.ds(4 * half + b, BLK, stride=8)
            out_ref[0, at, :] = tile[:, 128 * half : 128 * half + 128]

    t = z * X + x
    row = 2 * y + k

    @pl.when((row == lax.rem(t, 8)) & (lax.rem(a, 2) == t // 8))
    def _():
        for step in range(4):

            @pl.when(lax.rem(y - step + 4, 4) == a // 2)
            def _():
                both = own[step][1].astype(jnp.float32) + other[step][1].astype(jnp.float32)
                for half in range(2):
                    at = pl.ds(4 * half + a // 2, BLK, stride=8)
                    out_ref[0, at, :] = out_ref[0, at, :] + both[:, 128 * half : 128 * half + 128]


def limits(mib, flops=0, moved=0):
    return dict(
        compiler_params=pltpu.CompilerParams(vmem_limit_bytes=mib * 2**20),
        cost_estimate=pl.CostEstimate(flops=flops, bytes_accessed=moved, transcendentals=0),
    )


def assemble(parent_front, generators, diagonal_blocks, coupling, block_map, valid_rows):
    bf16 = jnp.bfloat16
    vmem = pl.BlockSpec(memory_space=pltpu.VMEM)
    hbm = pl.BlockSpec(memory_space=pltpu.HBM)
    block_map, valid_rows, generators, diagonal_blocks, coupling = (
        pltpu.with_memory_space_constraint(v, pltpu.HBM)
        for v in (block_map, valid_rows, generators, diagonal_blocks, coupling)
    )
    tables = [pltpu.SMEM(block_map.shape, jnp.int32)] * 2
    loc, rem, send = pl.pallas_call(
        rows_kernel,
        out_shape=(
            jax.ShapeDtypeStruct((2, BLK, BLK), bf16),
            jax.ShapeDtypeStruct((3, 2, 2, QUART, BLK), bf16),
            jax.ShapeDtypeStruct((14, 2 * QUART, BLK), bf16),
        ),
        in_specs=[hbm] * 3,
        out_specs=(vmem,) * 3,
        scratch_shapes=tables + [pltpu.VMEM(generators.shape, bf16), pltpu.SemaphoreType.DMA((3,))],
        **limits(8, 10**6, 2**21),
    )(block_map, valid_rows, generators)
    col = pl.pallas_call(
        column_kernel,
        out_shape=jax.ShapeDtypeStruct((2, BLK, BLK), bf16),
        in_specs=[hbm] * 5,
        out_specs=vmem,
        scratch_shapes=tables + [pltpu.VMEM((BLK, BLK), bf16)] * 3 + [pltpu.SemaphoreType.DMA((5,))],
        **limits(4, 2 * BLK**3, 2**19),
    )(block_map, valid_rows, generators, diagonal_blocks, coupling)

    flip = lambda y, k, z, x: (y, 1 - k, z, x)
    swap = shift(send, flip)
    got = {}
    for step in (1, 3, 2):
        there = swap[2 * step - 2 : 2 * step].reshape(2, 2, QUART, BLK).swapaxes(0, 1)
        payload = jnp.concatenate([rem[step - 1], there], axis=1)
        got[step] = shift(payload, lambda y, k, z, x, n=step: (y + n, k, z, x))
    cols = [col] + [shift(col, lambda y, k, z, x, n=n: (y + n, k, z, x)) for n in (1, 2, 3)]
    others = [shift(c, flip) for c in cols]
    for_x = jnp.stack([got[n][0] for n in (1, 2, 3)])
    for_z = jnp.stack([got[n][1] for n in (1, 2, 3)])
    xs = [shift(for_x, lambda y, k, z, x, n=n: (y, k, z, x + n)) for n in (1, 2, 3)]
    zs = [shift(for_z, lambda y, k, z, x, n=n: (y, k, z + n, x)) for n in (1, 2, 3)]

    a_count = parent_front.shape[0]
    flat = parent_front.reshape(a_count, BLK, 4, 2, 128).transpose(0, 1, 3, 2, 4).reshape(a_count, BLK * 8, 128)
    block = pl.BlockSpec((1, BLK * 8, 128), lambda a: (a, 0, 0))
    front = pl.pallas_call(
        fetch_kernel,
        grid=(a_count,),
        out_shape=jax.ShapeDtypeStruct((a_count, 4, BLK, BLK), jnp.float32),
        in_specs=[block],
        out_specs=vmem,
        **limits(16, 10**9, 2**23),
    )(flat)
    joined = pl.pallas_call(
        join_kernel,
        grid=(a_count,),
        out_shape=jax.ShapeDtypeStruct(flat.shape, jnp.float32),
        in_specs=[vmem] * 20,
        out_specs=block,
        scratch_shapes=[
            pltpu.VMEM((a_count, BLK, 2 * BLK), bf16),
            pltpu.VMEM((4, 2 * BLK, BLK), bf16),
        ],
        **limits(24, 2**31, 2**24),
    )(front, loc, swap, got[1], got[2], got[3], *xs, *zs, *cols, *others)
    return joined.reshape(a_count, BLK, 2, 4, 128).transpose(0, 1, 3, 2, 4).reshape(parent_front.shape)


def solution(mesh):
    in_specs = (P(None, "row", None, "col"), P("row", None, None), P("row", None, None), P(), P(), P())
    out_specs = P(None, "row", None, "col")
    return jax.shard_map(assemble, mesh=mesh, in_specs=in_specs, out_specs=out_specs, check_vma=False)
```

```python
import jax
import jax.numpy as jnp
from jax import lax
from jax.experimental import pallas as pl
from jax.experimental.pallas import tpu as pltpu
from jax.sharding import PartitionSpec as P


Y, Z, X, BLK = 4, 4, 4, 256
QUART = BLK // 4
WIN, CG = 16, 12


def pairs(move):
    out = []
    for y in range(Y):
        for k in range(2):
            for z in range(Z):
                for x in range(X):
                    b = move(y, k, z, x)
                    source = (2 * y + k) * Z * X + z * X + x
                    target = (2 * (b[0] % Y) + b[1]) * Z * X + (b[2] % Z) * X + b[3] % X
                    out.append((source, target))
    return out


def shift(value, move):
    return lax.ppermute(value, ("row", "col"), pairs(move))


def where_am_i():
    row = lax.axis_index("row")
    col = lax.axis_index("col")
    return row // 2, row % 2, col // X, col % X


def keep(count, start, rows):
    ids = lax.broadcasted_iota(jnp.int32, (rows, BLK), 0) + start
    return ids < count


def pack_kernel(
    map_hbm, count_hbm, gen_hbm, diag_hbm, coup_hbm, loc_ref, rem_ref, send_ref, col_ref,
    map_ref, count_ref, gen_ref, diag_ref, coup_ref, sems,
):
    y, k, z, x = where_am_i()
    base = y * CG
    tables = [
        pltpu.make_async_copy(map_hbm, map_ref, sems.at[0]),
        pltpu.make_async_copy(count_hbm, count_ref, sems.at[1]),
    ]
    gens = pltpu.make_async_copy(gen_hbm, gen_ref, sems.at[2])
    coup = pltpu.make_async_copy(coup_hbm.at[k], coup_ref, sems.at[3])
    for copy in tables + [gens, coup]:
        copy.start()
    zero = jnp.zeros((), jnp.bfloat16)
    loc_ref[...] = jnp.zeros_like(loc_ref)
    rem_ref[...] = jnp.zeros_like(rem_ref)
    send_ref[...] = jnp.zeros_like(send_ref)
    for copy in tables:
        copy.wait()

    target = y * WIN + z * X + x
    which = jnp.int32(0)
    kept = jnp.int32(0)
    for i in range(CG):
        hit = map_ref[k, base + i] == target
        which = jnp.where(hit, i, which)
        kept = jnp.where(hit, count_ref[k, base + i], kept)
    diag = pltpu.make_async_copy(diag_hbm.at[which], diag_ref, sems.at[4])
    diag.start()
    gens.wait()
    start = pl.multiple_of(QUART * jnp.where(k == 0, x, z), QUART)
    start_theirs = pl.multiple_of(QUART * jnp.where(k == 0, z, x), QUART)

    def one(i, carry):
        w = map_ref[k, base + i] - y * WIN
        count = count_ref[k, base + i]
        mine = lax.rem(w, 2) == k
        m = w // 8
        step = lax.rem(lax.rem(w // 2, 4) - y + 4, 4)

        @pl.when(step == 0)
        def _():
            full = jnp.where(keep(count, 0, BLK), gen_ref[i], zero)

            @pl.when(mine)
            def _():
                loc_ref[m] = full

            @pl.when(jnp.logical_not(mine))
            def _():
                for part in range(4):
                    send_ref[6 + 4 * m + part] = full[QUART * part : QUART * part + QUART]

        @pl.when(step > 0)
        def _():
            at = pl.multiple_of(jnp.where(mine, start, start_theirs), QUART)
            piece = jnp.where(keep(count, at, QUART), gen_ref[i, pl.ds(at, QUART), :], zero)

            @pl.when(mine)
            def _():
                rem_ref[step - 1, m] = piece

            @pl.when(jnp.logical_not(mine))
            def _():
                send_ref[2 * (step - 1) + m] = piece

        return carry

    lax.fori_loop(0, CG, one, 0)
    coup.wait()
    full = jnp.where(keep(kept, 0, BLK), gen_ref[which], zero)
    col_ref[0] = lax.dot_general(
        coup_ref[...], full, (((0,), (1,)), ((), ())), preferred_element_type=jnp.float32
    ).astype(jnp.bfloat16)
    diag.wait()
    lanes = lax.broadcasted_iota(jnp.int32, (BLK, BLK), 1) < kept
    col_ref[1] = jnp.where(keep(kept, 0, BLK) & lanes, diag_ref[...], zero)


def fetch_kernel(par_hbm, out_ref, buf_ref, sems):
    count = buf_ref.shape[0]
    y = where_am_i()[0]
    wanted = [2 * lax.rem(y - STEPS[i // 2] + 4, 4) + i % 2 for i in range(count)]
    copies = [pltpu.make_async_copy(par_hbm.at[a], buf_ref.at[i], sems.at[i]) for i, a in enumerate(wanted)]
    for copy in copies:
        copy.start()
    for a in range(count):
        copies[a].wait()
        for b in range(4):
            for half in range(2):
                at = pl.ds(4 * half + b, BLK, stride=8)
                out_ref[a, b, :, 128 * half : 128 * half + 128] = buf_ref[a, at, :]


STEPS = (0, 1, 3, 2)


def join_kernel(
    front_ref, loc_ref, swap_ref, g0, near1, far1, g2, near3, far3,
    col_ref, colswap_ref, c1, c2, fc1, fc2, out_hbm, rows_ref, cols_ref, diag_ref, out_ref, sems,
):
    y, k, z, x = where_am_i()
    t = z * X + x
    crossing = 2 * y + k == lax.rem(t, 8)
    group = [lax.rem(y - step + 4, 4) for step in STEPS]
    count = out_ref.shape[0]
    back = lax.rem(y + 3 + 2 * k, 4)
    ahead = lax.rem(y + 1 + 2 * k, 4)
    across = lax.rem(y + 2, 4)
    homes = (
        (y, col_ref.at[0], col_ref.at[1], colswap_ref.at[0], colswap_ref.at[1]),
        (back, c1.at[0], c1.at[1], c1.at[2], c1.at[3]),
        (ahead, fc1.at[2], fc1.at[3], fc1.at[0], fc1.at[1]),
        (across, c2.at[0], c2.at[1], fc2.at[0], fc2.at[1]),
    )

    for s, proj, diag, proj2, diag2 in homes:
        cols_ref[s, :BLK] = proj[...]
        cols_ref[s, BLK:] = proj2[...]
        diag_ref[s] = diag[...].astype(jnp.float32) + diag2[...].astype(jnp.float32)

    q = jnp.where(k == 0, x, z)
    spots = [pl.multiple_of(QUART * lax.rem(q - n + 4, 4), QUART) for n in range(4)]
    copies = []
    for i in range(count):
        m = i % 2
        if i < 2:
            rows_ref[i, :, :BLK] = loc_ref[m]
            for n in range(4):
                rows_ref[i, QUART * n : QUART * n + QUART, BLK:] = swap_ref[6 + 4 * m + n]
        else:
            j = i // 2 - 1
            quarters = [g0.at[j], near1.at[j] if j < 2 else far1, g2.at[j], near3.at[j] if j < 2 else far3]
            for at, quarter in zip(spots, quarters):
                rows_ref[i, pl.ds(at, QUART), :BLK] = quarter[0, m]
                rows_ref[i, pl.ds(at, QUART), BLK:] = quarter[1, m]
        left = rows_ref[i]
        s = group[i // 2]
        amount = jnp.where(crossing & (m == t // 8), 1.0, 0.0)
        for j in range(4):
            b = lax.rem(s + j, 4)
            tile = front_ref[i, b] + jnp.dot(left, cols_ref[b], preferred_element_type=jnp.float32)
            if j == 0:
                tile = tile + amount * diag_ref[s]
            for half in range(2):
                out_ref[i, pl.ds(4 * half + b, BLK, stride=8), :] = tile[:, 128 * half : 128 * half + 128]

        copy = pltpu.make_async_copy(out_ref.at[i], out_hbm.at[2 * s + m], sems.at[i])
        copy.start()
        copies.append(copy)
    for copy in copies:
        copy.wait()


def limits(mib, flops=0, moved=0):
    return dict(
        compiler_params=pltpu.CompilerParams(vmem_limit_bytes=mib * 2**20),
        cost_estimate=pl.CostEstimate(flops=flops, bytes_accessed=moved, transcendentals=0),
    )


def assemble(parent_front, generators, diagonal_blocks, coupling, block_map, valid_rows):
    bf16 = jnp.bfloat16
    vmem = pl.BlockSpec(memory_space=pltpu.VMEM)
    hbm = pl.BlockSpec(memory_space=pltpu.HBM)
    inputs = [
        pltpu.with_memory_space_constraint(v, pltpu.HBM)
        for v in (block_map, valid_rows, generators, diagonal_blocks, coupling)
    ]
    loc, rem, send, col = pl.pallas_call(
        pack_kernel,
        out_shape=(
            jax.ShapeDtypeStruct((2, BLK, BLK), bf16),
            jax.ShapeDtypeStruct((3, 2, QUART, BLK), bf16),
            jax.ShapeDtypeStruct((14, QUART, BLK), bf16),
            jax.ShapeDtypeStruct((2, BLK, BLK), bf16),
        ),
        in_specs=[hbm] * 5,
        out_specs=(vmem,) * 4,
        scratch_shapes=[
            pltpu.SMEM(block_map.shape, jnp.int32),
            pltpu.SMEM(valid_rows.shape, jnp.int32),
            pltpu.VMEM(generators.shape, bf16),
            pltpu.VMEM((BLK, BLK), bf16),
            pltpu.VMEM((BLK, BLK), bf16),
            pltpu.SemaphoreType.DMA((5,)),
        ],
        **limits(8, 2 * BLK**3, 2**21),
    )(*inputs)

    flip = lambda y, k, z, x: (y, 1 - k, z, x)
    swap = shift(send, flip)
    colswap = shift(col, flip)
    got = {}
    for n in (1, 3, 2):
        payload = jnp.stack([rem[n - 1], swap[2 * n - 2 : 2 * n]])
        got[n] = shift(payload, lambda y, k, z, x, n=n: (y + n, k, z, x))
    both = jnp.concatenate([col, colswap])
    c1 = shift(both, lambda y, k, z, x: (y + 1 - 2 * k, k, z, x))
    c2 = shift(col, lambda y, k, z, x: (y + 2, k, z, x))
    near = jnp.stack([got[1], got[3]])
    far = got[2]
    mine = jnp.concatenate([near, far[None]])

    def gather(value, n):
        return shift(value, lambda y, k, z, x: (y, k, z + n * k, x + n * (1 - k)))

    near1 = gather(near, 1)
    near3 = gather(near, 3)
    both2 = gather(mine, 2)
    far1 = gather(far, 1)
    far3 = gather(far, 3)
    pieces = [mine, near1, far1, both2, near3, far3]
    fc1 = shift(c1, flip)
    fc2 = shift(c2, flip)

    a_count = parent_front.shape[0]
    flat = parent_front.reshape(a_count, BLK, 4, 2, 128).transpose(0, 1, 3, 2, 4).reshape(a_count, BLK * 8, 128)
    flat = pltpu.with_memory_space_constraint(flat, pltpu.HBM)
    front = pl.pallas_call(
        fetch_kernel,
        out_shape=jax.ShapeDtypeStruct((a_count, 4, BLK, BLK), jnp.float32),
        in_specs=[hbm],
        out_specs=vmem,
        scratch_shapes=[pltpu.VMEM(flat.shape, jnp.float32), pltpu.SemaphoreType.DMA((a_count,))],
        **limits(20, 10**9, 2**23),
    )(flat)
    joined = pl.pallas_call(
        join_kernel,
        out_shape=jax.ShapeDtypeStruct(flat.shape, jnp.float32),
        in_specs=[vmem] * 15,
        out_specs=hbm,
        scratch_shapes=[
            pltpu.VMEM((a_count, BLK, 2 * BLK), bf16),
            pltpu.VMEM((4, 2 * BLK, BLK), bf16),
            pltpu.VMEM((4, BLK, BLK), jnp.float32),
            pltpu.VMEM(flat.shape, jnp.float32),
            pltpu.SemaphoreType.DMA((a_count,)),
        ],
        **limits(24, 2**31, 2**24),
    )(front, loc, swap, *pieces, col, colswap, c1, c2, fc1, fc2)
    return joined.reshape(a_count, BLK, 2, 4, 128).transpose(0, 1, 3, 2, 4).reshape(parent_front.shape)


def solution(mesh):
    in_specs = (P(None, "row", None, "col"), P("row", None, None), P("row", None, None), P(), P(), P())
    out_specs = P(None, "row", None, "col")
    return jax.shard_map(assemble, mesh=mesh, in_specs=in_specs, out_specs=out_specs, check_vma=False)
```

```python
import jax
import jax.numpy as jnp
from jax import lax
from jax.experimental import pallas as pl
from jax.experimental.pallas import tpu as pltpu
from jax.sharding import PartitionSpec as P


Y, Z, X, BLK = 4, 4, 4, 256
QUART = BLK // 4
WIN, CG = 16, 12


def pairs(move):
    out = []
    for y in range(Y):
        for k in range(2):
            for z in range(Z):
                for x in range(X):
                    b = move(y, k, z, x)
                    source = (2 * y + k) * Z * X + z * X + x
                    target = (2 * (b[0] % Y) + b[1]) * Z * X + (b[2] % Z) * X + b[3] % X
                    out.append((source, target))
    return out


def shift(value, move):
    return lax.ppermute(value, ("row", "col"), pairs(move))


def where_am_i():
    row = lax.axis_index("row")
    col = lax.axis_index("col")
    return row // 2, row % 2, col // X, col % X


def keep(count, start, rows):
    ids = lax.broadcasted_iota(jnp.int32, (rows, BLK), 0) + start
    return ids < count


def pack_kernel(
    map_hbm, count_hbm, gen_hbm, diag_hbm, coup_hbm, loc_ref, rem_ref, send_ref, col_ref,
    map_ref, count_ref, slot_ref, gen_ref, diag_ref, coup_ref, sems,
):
    y, k, z, x = where_am_i()
    base = y * CG
    tables = [
        pltpu.make_async_copy(map_hbm, map_ref, sems.at[0]),
        pltpu.make_async_copy(count_hbm, count_ref, sems.at[1]),
    ]
    gens = pltpu.make_async_copy(gen_hbm, gen_ref, sems.at[2])
    coup = pltpu.make_async_copy(coup_hbm.at[k], coup_ref, sems.at[3])
    for copy in tables + [gens, coup]:
        copy.start()
    zero = jnp.zeros((), jnp.bfloat16)
    for copy in tables:
        copy.wait()

    for w in range(WIN):
        slot_ref[w] = -1
    for i in range(CG):
        slot_ref[map_ref[k, base + i] - y * WIN] = i

    def at_slot(w):
        i = slot_ref[w]
        block = jnp.maximum(i, 0)
        return block, jnp.where(i >= 0, count_ref[k, base + block], 0)

    which, kept = at_slot(z * X + x)
    diag = pltpu.make_async_copy(diag_hbm.at[which], diag_ref, sems.at[4])
    diag.start()
    gens.wait()
    starts = (QUART * jnp.where(k == 0, x, z), QUART * jnp.where(k == 0, z, x))
    for step in range(4):
        chip = lax.rem(y + step, 4)
        for theirs in range(2):
            start = pl.multiple_of(starts[theirs], QUART)
            for m in range(2):
                i, count = at_slot(8 * m + 2 * chip + (k if theirs == 0 else 1 - k))
                if step == 0:
                    full = jnp.where(keep(count, 0, BLK), gen_ref[i], zero)
                    if theirs == 0:
                        loc_ref[m] = full
                    else:
                        for part in range(4):
                            send_ref[6 + 4 * m + part] = full[QUART * part : QUART * part + QUART]
                else:
                    piece = jnp.where(keep(count, start, QUART), gen_ref[i, pl.ds(start, QUART), :], zero)
                    if theirs == 0:
                        rem_ref[step - 1, m] = piece
                    else:
                        send_ref[2 * (step - 1) + m] = piece
    coup.wait()
    full = jnp.where(keep(kept, 0, BLK), gen_ref[which], zero)
    col_ref[0] = lax.dot_general(
        coup_ref[...], full, (((0,), (1,)), ((), ())), preferred_element_type=jnp.float32
    ).astype(jnp.bfloat16)
    diag.wait()
    lanes = lax.broadcasted_iota(jnp.int32, (BLK, BLK), 1) < kept
    col_ref[1] = jnp.where(keep(kept, 0, BLK) & lanes, diag_ref[...], zero)


def fetch_kernel(par_hbm, out_ref, buf_ref, sems):
    count = buf_ref.shape[0]
    y = where_am_i()[0]
    wanted = [2 * lax.rem(y - STEPS[i // 2] + 4, 4) + i % 2 for i in range(count)]
    copies = [pltpu.make_async_copy(par_hbm.at[a], buf_ref.at[i], sems.at[i]) for i, a in enumerate(wanted)]
    for copy in copies:
        copy.start()
    for a in range(count):
        copies[a].wait()
        for b in range(4):
            for half in range(2):
                at = pl.ds(4 * half + b, BLK, stride=8)
                out_ref[a, b, :, 128 * half : 128 * half + 128] = buf_ref[a, at, :]


STEPS = (0, 1, 3, 2)


def join_kernel(
    front_ref, loc_ref, swap_ref, g0, near1, far1, g2, near3, far3,
    col_ref, colswap_ref, c1, c2, fc1, fc2, out_hbm, rows_ref, cols_ref, diag_ref, out_ref, sems,
):
    y, k, z, x = where_am_i()
    t = z * X + x
    crossing = 2 * y + k == lax.rem(t, 8)
    group = [lax.rem(y - step + 4, 4) for step in STEPS]
    count = out_ref.shape[0]
    back = lax.rem(y + 3 + 2 * k, 4)
    ahead = lax.rem(y + 1 + 2 * k, 4)
    across = lax.rem(y + 2, 4)
    homes = (
        (y, col_ref.at[0], col_ref.at[1], colswap_ref.at[0], colswap_ref.at[1]),
        (back, c1.at[0], c1.at[1], c1.at[2], c1.at[3]),
        (ahead, fc1.at[2], fc1.at[3], fc1.at[0], fc1.at[1]),
        (across, c2.at[0], c2.at[1], fc2.at[0], fc2.at[1]),
    )

    for s, proj, diag, proj2, diag2 in homes:
        cols_ref[s, :BLK] = proj[...]
        cols_ref[s, BLK:] = proj2[...]
        diag_ref[s] = diag[...].astype(jnp.float32) + diag2[...].astype(jnp.float32)

    q = jnp.where(k == 0, x, z)
    spots = [pl.multiple_of(QUART * lax.rem(q - n + 4, 4), QUART) for n in range(4)]
    copies = []
    for i in range(count):
        m = i % 2
        if i < 2:
            rows_ref[i, :, :BLK] = loc_ref[m]
            for n in range(4):
                rows_ref[i, QUART * n : QUART * n + QUART, BLK:] = swap_ref[6 + 4 * m + n]
        else:
            j = i // 2 - 1
            quarters = [g0.at[j], near1.at[j] if j < 2 else far1, g2.at[j], near3.at[j] if j < 2 else far3]
            for at, quarter in zip(spots, quarters):
                rows_ref[i, pl.ds(at, QUART), :BLK] = quarter[0, m]
                rows_ref[i, pl.ds(at, QUART), BLK:] = quarter[1, m]
        left = rows_ref[i]
        s = group[i // 2]
        amount = jnp.where(crossing & (m == t // 8), 1.0, 0.0)
        for j in range(4):
            b = lax.rem(s + j, 4)
            tile = front_ref[i, b] + jnp.dot(left, cols_ref[b], preferred_element_type=jnp.float32)
            if j == 0:
                tile = tile + amount * diag_ref[s]
            for half in range(2):
                out_ref[i, pl.ds(4 * half + b, BLK, stride=8), :] = tile[:, 128 * half : 128 * half + 128]

        copy = pltpu.make_async_copy(out_ref.at[i], out_hbm.at[2 * s + m], sems.at[i])
        copy.start()
        copies.append(copy)
    for copy in copies:
        copy.wait()


def limits(mib, flops=0, moved=0):
    return dict(
        compiler_params=pltpu.CompilerParams(vmem_limit_bytes=mib * 2**20),
        cost_estimate=pl.CostEstimate(flops=flops, bytes_accessed=moved, transcendentals=0),
    )


def assemble(parent_front, generators, diagonal_blocks, coupling, block_map, valid_rows):
    bf16 = jnp.bfloat16
    vmem = pl.BlockSpec(memory_space=pltpu.VMEM)
    hbm = pl.BlockSpec(memory_space=pltpu.HBM)
    inputs = [
        pltpu.with_memory_space_constraint(v, pltpu.HBM)
        for v in (block_map, valid_rows, generators, diagonal_blocks, coupling)
    ]
    loc, rem, send, col = pl.pallas_call(
        pack_kernel,
        out_shape=(
            jax.ShapeDtypeStruct((2, BLK, BLK), bf16),
            jax.ShapeDtypeStruct((3, 2, QUART, BLK), bf16),
            jax.ShapeDtypeStruct((14, QUART, BLK), bf16),
            jax.ShapeDtypeStruct((2, BLK, BLK), bf16),
        ),
        in_specs=[hbm] * 5,
        out_specs=(vmem,) * 4,
        scratch_shapes=[
            pltpu.SMEM(block_map.shape, jnp.int32),
            pltpu.SMEM(valid_rows.shape, jnp.int32),
            pltpu.SMEM((WIN,), jnp.int32),
            pltpu.VMEM(generators.shape, bf16),
            pltpu.VMEM((BLK, BLK), bf16),
            pltpu.VMEM((BLK, BLK), bf16),
            pltpu.SemaphoreType.DMA((5,)),
        ],
        **limits(8, 2 * BLK**3, 2**21),
    )(*inputs)

    flip = lambda y, k, z, x: (y, 1 - k, z, x)
    swap = shift(send, flip)
    colswap = shift(col, flip)
    got = {}
    for n in (1, 3, 2):
        payload = jnp.stack([rem[n - 1], swap[2 * n - 2 : 2 * n]])
        got[n] = shift(payload, lambda y, k, z, x, n=n: (y + n, k, z, x))
    both = jnp.concatenate([col, colswap])
    c1 = shift(both, lambda y, k, z, x: (y + 1 - 2 * k, k, z, x))
    c2 = shift(col, lambda y, k, z, x: (y + 2, k, z, x))
    near = jnp.stack([got[1], got[3]])
    far = got[2]
    mine = jnp.concatenate([near, far[None]])

    def gather(value, n):
        return shift(value, lambda y, k, z, x: (y, k, z + n * k, x + n * (1 - k)))

    near1 = gather(near, 1)
    near3 = gather(near, 3)
    both2 = gather(mine, 2)
    far1 = gather(far, 1)
    far3 = gather(far, 3)
    pieces = [mine, near1, far1, both2, near3, far3]
    fc1 = shift(c1, flip)
    fc2 = shift(c2, flip)

    a_count = parent_front.shape[0]
    flat = parent_front.reshape(a_count, BLK, 4, 2, 128).transpose(0, 1, 3, 2, 4).reshape(a_count, BLK * 8, 128)
    flat = pltpu.with_memory_space_constraint(flat, pltpu.HBM)
    front = pl.pallas_call(
        fetch_kernel,
        out_shape=jax.ShapeDtypeStruct((a_count, 4, BLK, BLK), jnp.float32),
        in_specs=[hbm],
        out_specs=vmem,
        scratch_shapes=[pltpu.VMEM(flat.shape, jnp.float32), pltpu.SemaphoreType.DMA((a_count,))],
        **limits(20, 10**9, 2**23),
    )(flat)
    joined = pl.pallas_call(
        join_kernel,
        out_shape=jax.ShapeDtypeStruct(flat.shape, jnp.float32),
        in_specs=[vmem] * 15,
        out_specs=hbm,
        scratch_shapes=[
            pltpu.VMEM((a_count, BLK, 2 * BLK), bf16),
            pltpu.VMEM((4, 2 * BLK, BLK), bf16),
            pltpu.VMEM((4, BLK, BLK), jnp.float32),
            pltpu.VMEM(flat.shape, jnp.float32),
            pltpu.SemaphoreType.DMA((a_count,)),
        ],
        **limits(24, 2**31, 2**24),
    )(front, loc, swap, *pieces, col, colswap, c1, c2, fc1, fc2)
    return joined.reshape(a_count, BLK, 2, 4, 128).transpose(0, 1, 3, 2, 4).reshape(parent_front.shape)


def solution(mesh):
    in_specs = (P(None, "row", None, "col"), P("row", None, None), P("row", None, None), P(), P(), P())
    out_specs = P(None, "row", None, "col")
    return jax.shard_map(assemble, mesh=mesh, in_specs=in_specs, out_specs=out_specs, check_vma=False)
```

```python
import jax
import jax.numpy as jnp
from jax import lax
from jax.experimental import pallas as pl
from jax.experimental.pallas import tpu as pltpu
from jax.sharding import PartitionSpec as P


Y, Z, X, BLK = 4, 4, 4, 256
QUART = BLK // 4
WIN, CG = 16, 12


def pairs(move):
    out = []
    for y in range(Y):
        for k in range(2):
            for z in range(Z):
                for x in range(X):
                    b = move(y, k, z, x)
                    source = (2 * y + k) * Z * X + z * X + x
                    target = (2 * (b[0] % Y) + b[1]) * Z * X + (b[2] % Z) * X + b[3] % X
                    out.append((source, target))
    return out


def shift(value, move):
    return lax.ppermute(value, ("row", "col"), pairs(move))


def where_am_i():
    row = lax.axis_index("row")
    col = lax.axis_index("col")
    return row // 2, row % 2, col // X, col % X


def keep(count, start, rows):
    ids = lax.broadcasted_iota(jnp.int32, (rows, BLK), 0) + start
    return ids < count


def pack_kernel(
    map_hbm, count_hbm, gen_hbm, diag_hbm, coup_hbm, loc_ref, rem_ref, send_ref, col_ref,
    map_ref, count_ref, slot_ref, gen_ref, diag_ref, coup_ref, sems,
):
    y, k, z, x = where_am_i()
    base = y * CG
    tables = [
        pltpu.make_async_copy(map_hbm, map_ref, sems.at[0]),
        pltpu.make_async_copy(count_hbm, count_ref, sems.at[1]),
    ]
    gens = pltpu.make_async_copy(gen_hbm, gen_ref, sems.at[2])
    coup = pltpu.make_async_copy(coup_hbm.at[k], coup_ref, sems.at[3])
    for copy in tables + [gens, coup]:
        copy.start()
    zero = jnp.zeros((), jnp.bfloat16)
    for copy in tables:
        copy.wait()

    for w in range(WIN):
        slot_ref[w] = -1
    for i in range(CG):
        slot_ref[map_ref[k, base + i] - y * WIN] = i

    def at_slot(w):
        i = slot_ref[w]
        block = jnp.maximum(i, 0)
        return block, jnp.where(i >= 0, count_ref[k, base + block], 0)

    which, kept = at_slot(z * X + x)
    diag = pltpu.make_async_copy(diag_hbm.at[which], diag_ref, sems.at[4])
    diag.start()
    gens.wait()
    starts = (QUART * jnp.where(k == 0, x, z), QUART * jnp.where(k == 0, z, x))
    for step in range(4):
        chip = lax.rem(y + step, 4)
        for theirs in range(2):
            start = pl.multiple_of(starts[theirs], QUART)
            for m in range(2):
                i, count = at_slot(8 * m + 2 * chip + (k if theirs == 0 else 1 - k))
                if step == 0:
                    full = jnp.where(keep(count, 0, BLK), gen_ref[i], zero)
                    if theirs == 0:
                        loc_ref[m] = full
                    else:
                        for part in range(4):
                            send_ref[6 + 4 * m + part] = full[QUART * part : QUART * part + QUART]
                else:
                    piece = jnp.where(keep(count, start, QUART), gen_ref[i, pl.ds(start, QUART), :], zero)
                    core = k if theirs == 0 else 1 - k
                    turn = {1: core, 3: 1 - core, 2: 2}[step]
                    if theirs == 0:
                        rem_ref[turn, m] = piece
                    else:
                        send_ref[2 * turn + m] = piece
    coup.wait()
    full = jnp.where(keep(kept, 0, BLK), gen_ref[which], zero)
    col_ref[0] = lax.dot_general(
        coup_ref[...], full, (((0,), (1,)), ((), ())), preferred_element_type=jnp.float32
    ).astype(jnp.bfloat16)
    diag.wait()
    lanes = lax.broadcasted_iota(jnp.int32, (BLK, BLK), 1) < kept
    col_ref[1] = jnp.where(keep(kept, 0, BLK) & lanes, diag_ref[...], zero)


def groups(y, k):
    return [y, lax.rem(y + 3 + 2 * k, 4), lax.rem(y + 1 + 2 * k, 4), lax.rem(y + 2, 4)]


def fetch_kernel(par_hbm, out_ref, buf_ref, sems):
    count = buf_ref.shape[0]
    y, k, _, _ = where_am_i()
    group = groups(y, k)
    wanted = [2 * group[i // 2] + i % 2 for i in range(count)]
    copies = [pltpu.make_async_copy(par_hbm.at[a], buf_ref.at[i], sems.at[i]) for i, a in enumerate(wanted)]
    for copy in copies:
        copy.start()
    for a in range(count):
        copies[a].wait()
        for b in range(4):
            for half in range(2):
                at = pl.ds(4 * half + b, BLK, stride=8)
                out_ref[a, b, :, 128 * half : 128 * half + 128] = buf_ref[a, at, :]


def join_kernel(
    front_ref, loc_ref, swap_ref, g0, near1, far1, g2, near3, far3,
    col_ref, colswap_ref, c1, c2, fc1, fc2, out_hbm, rows_ref, cols_ref, diag_ref, out_ref, sems,
):
    y, k, z, x = where_am_i()
    t = z * X + x
    crossing = 2 * y + k == lax.rem(t, 8)
    group = groups(y, k)
    count = out_ref.shape[0]
    _, back, ahead, across = group
    homes = (
        (y, col_ref.at[0], col_ref.at[1], colswap_ref.at[0], colswap_ref.at[1]),
        (back, c1.at[0], c1.at[1], c1.at[2], c1.at[3]),
        (ahead, fc1.at[2], fc1.at[3], fc1.at[0], fc1.at[1]),
        (across, c2.at[0], c2.at[1], fc2.at[0], fc2.at[1]),
    )

    for s, proj, diag, proj2, diag2 in homes:
        cols_ref[s, :BLK] = proj[...]
        cols_ref[s, BLK:] = proj2[...]
        diag_ref[s] = diag[...].astype(jnp.float32) + diag2[...].astype(jnp.float32)

    q = jnp.where(k == 0, x, z)
    spots = [pl.multiple_of(QUART * lax.rem(q - n + 4, 4), QUART) for n in range(4)]
    copies = []
    for i in range(count):
        m = i % 2
        if i < 2:
            rows_ref[i, :, :BLK] = loc_ref[m]
            for n in range(4):
                rows_ref[i, QUART * n : QUART * n + QUART, BLK:] = swap_ref[6 + 4 * m + n]
        else:
            j = i // 2 - 1
            quarters = [g0.at[j], near1.at[j] if j < 2 else far1, g2.at[j], near3.at[j] if j < 2 else far3]
            for at, quarter in zip(spots, quarters):
                rows_ref[i, pl.ds(at, QUART), :BLK] = quarter[0, m]
                rows_ref[i, pl.ds(at, QUART), BLK:] = quarter[1, m]
        left = rows_ref[i]
        s = group[i // 2]
        amount = jnp.where(crossing & (m == t // 8), 1.0, 0.0)
        for j in range(4):
            b = lax.rem(s + j, 4)
            tile = front_ref[i, b] + jnp.dot(left, cols_ref[b], preferred_element_type=jnp.float32)
            if j == 0:
                tile = tile + amount * diag_ref[s]
            for half in range(2):
                out_ref[i, pl.ds(4 * half + b, BLK, stride=8), :] = tile[:, 128 * half : 128 * half + 128]

        copy = pltpu.make_async_copy(out_ref.at[i], out_hbm.at[2 * s + m], sems.at[i])
        copy.start()
        copies.append(copy)
    for copy in copies:
        copy.wait()


def limits(mib, flops=0, moved=0):
    return dict(
        compiler_params=pltpu.CompilerParams(vmem_limit_bytes=mib * 2**20),
        cost_estimate=pl.CostEstimate(flops=flops, bytes_accessed=moved, transcendentals=0),
    )


def assemble(parent_front, generators, diagonal_blocks, coupling, block_map, valid_rows):
    bf16 = jnp.bfloat16
    vmem = pl.BlockSpec(memory_space=pltpu.VMEM)
    hbm = pl.BlockSpec(memory_space=pltpu.HBM)
    inputs = [
        pltpu.with_memory_space_constraint(v, pltpu.HBM)
        for v in (block_map, valid_rows, generators, diagonal_blocks, coupling)
    ]
    loc, rem, send, col = pl.pallas_call(
        pack_kernel,
        out_shape=(
            jax.ShapeDtypeStruct((2, BLK, BLK), bf16),
            jax.ShapeDtypeStruct((3, 2, QUART, BLK), bf16),
            jax.ShapeDtypeStruct((14, QUART, BLK), bf16),
            jax.ShapeDtypeStruct((2, BLK, BLK), bf16),
        ),
        in_specs=[hbm] * 5,
        out_specs=(vmem,) * 4,
        scratch_shapes=[
            pltpu.SMEM(block_map.shape, jnp.int32),
            pltpu.SMEM(valid_rows.shape, jnp.int32),
            pltpu.SMEM((WIN,), jnp.int32),
            pltpu.VMEM(generators.shape, bf16),
            pltpu.VMEM((BLK, BLK), bf16),
            pltpu.VMEM((BLK, BLK), bf16),
            pltpu.SemaphoreType.DMA((5,)),
        ],
        **limits(8, 2 * BLK**3, 2**21),
    )(*inputs)

    flip = lambda y, k, z, x: (y, 1 - k, z, x)
    swap = shift(send, flip)
    colswap = shift(col, flip)
    ways = (
        lambda y, k, z, x: (y + 1 - 2 * k, k, z, x),
        lambda y, k, z, x: (y - 1 + 2 * k, k, z, x),
        lambda y, k, z, x: (y + 2, k, z, x),
    )
    got = [shift(jnp.stack([rem[n], swap[2 * n : 2 * n + 2]]), ways[n]) for n in range(3)]
    both = jnp.concatenate([col, colswap])
    c1 = shift(both, lambda y, k, z, x: (y + 1 - 2 * k, k, z, x))
    c2 = shift(col, lambda y, k, z, x: (y + 2, k, z, x))
    near = jnp.stack([got[0], got[1]])
    far = got[2]
    mine = jnp.concatenate([near, far[None]])

    def gather(value, n):
        return shift(value, lambda y, k, z, x: (y, k, z + n * k, x + n * (1 - k)))

    near1 = gather(near, 1)
    near3 = gather(near, 3)
    both2 = gather(mine, 2)
    far1 = gather(far, 1)
    far3 = gather(far, 3)
    pieces = [mine, near1, far1, both2, near3, far3]
    fc1 = shift(c1, flip)
    fc2 = shift(c2, flip)

    a_count = parent_front.shape[0]
    flat = parent_front.reshape(a_count, BLK, 4, 2, 128).transpose(0, 1, 3, 2, 4).reshape(a_count, BLK * 8, 128)
    flat = pltpu.with_memory_space_constraint(flat, pltpu.HBM)
    front = pl.pallas_call(
        fetch_kernel,
        out_shape=jax.ShapeDtypeStruct((a_count, 4, BLK, BLK), jnp.float32),
        in_specs=[hbm],
        out_specs=vmem,
        scratch_shapes=[pltpu.VMEM(flat.shape, jnp.float32), pltpu.SemaphoreType.DMA((a_count,))],
        **limits(20, 10**9, 2**23),
    )(flat)
    joined = pl.pallas_call(
        join_kernel,
        out_shape=jax.ShapeDtypeStruct(flat.shape, jnp.float32),
        in_specs=[vmem] * 15,
        out_specs=hbm,
        scratch_shapes=[
            pltpu.VMEM((a_count, BLK, 2 * BLK), bf16),
            pltpu.VMEM((4, 2 * BLK, BLK), bf16),
            pltpu.VMEM((4, BLK, BLK), jnp.float32),
            pltpu.VMEM(flat.shape, jnp.float32),
            pltpu.SemaphoreType.DMA((a_count,)),
        ],
        **limits(24, 2**31, 2**24),
    )(front, loc, swap, *pieces, col, colswap, c1, c2, fc1, fc2)
    return joined.reshape(a_count, BLK, 2, 4, 128).transpose(0, 1, 3, 2, 4).reshape(parent_front.shape)


def solution(mesh):
    in_specs = (P(None, "row", None, "col"), P("row", None, None), P("row", None, None), P(), P(), P())
    out_specs = P(None, "row", None, "col")
    return jax.shard_map(assemble, mesh=mesh, in_specs=in_specs, out_specs=out_specs, check_vma=False)
```
